8 devices in a mesh: dp: 2 (over y, z), tp: 4 (over x, core).
Axes of the slice: x: 2, y: 2, z: 1, core: 2. Of those that a mesh axis runs over, the one named last changes fastest.
Arguments:
- x: bfloat16 [256, 4096], P('dp'), parts along dimension 0
- w_gate: bfloat16 [4096, 10240], P(None, 'tp')
- w_up: bfloat16 [4096, 10240], P(None, 'tp')
- w_down: bfloat16 [10240, 4096], P('tp')
Outputs:
- output: bfloat16 [256, 4096], P('dp'), parts along dimension 0
There are 2 independent parts. The reference program is written for one: setup_inputs(seed, part) draws one part's arguments, and reference() takes and returns one part's arrays. A program takes and returns all parts, laid end to end along the dimension named above; an argument that names none is the same for every part.
All inputs are finite; a program needn't handle non-finite values.
Results may differ from the reference program's by a relative error of at most 0.016.
Values are sent between devices in bfloat16 or wider.
A program may use at most 2 GiB of HBM per device.

```python
import jax
import jax.numpy as jnp

ROWS = 128
D = 4096
FF = 10240


def setup_inputs(seed: int = 0, part: int = 0) -> dict:
    kx, kg, ku, kd = jax.random.split(jax.random.key(seed), 4)
    drawn = {
        "x": jax.random.normal(jax.random.fold_in(kx, part), (ROWS, D), jnp.float32),
        "w_gate": jax.random.normal(kg, (D, FF), jnp.float32) * D**-0.5,
        "w_up": jax.random.normal(ku, (D, FF), jnp.float32) * D**-0.5,
        "w_down": jax.random.normal(kd, (FF, D), jnp.float32) * FF**-0.5,
    }
    return {k: v.astype(jnp.bfloat16) for k, v in drawn.items()}


def reference(x, w_gate, w_up, w_down):
    gate = jnp.dot(x, w_gate, preferred_element_type=jnp.float32)
    up = jnp.dot(x, w_up, preferred_element_type=jnp.float32)
    hidden = (jax.nn.gelu(gate) * up).astype(jnp.bfloat16)
    return jnp.dot(hidden, w_down, preferred_element_type=jnp.float32).astype(jnp.bfloat16)
```

```python
import functools

import jax
import jax.numpy as jnp
from jax import lax
from jax.experimental import pallas as pl
from jax.experimental.pallas import tpu as pltpu
from jax.sharding import PartitionSpec as P

MESH = pl.DeviceIdType.MESH
BF16 = jnp.bfloat16
F32 = jnp.float32

B1 = 256
KQ = 4
RING = 4
B2 = 256
LAG = 3


def kernel(
    x_hbm, wg_hbm, wu_hbm, wd_hbm, y_ref,
    xv, wgv, wuv, wdv, hid, term, pair_out, pair_in, chip_out, chip_in,
    x_sem, g_sem, u_sem, d_sem,
    ps_sem, pr_sem, cs_sem, cr_sem, ys_sem, yr_sem,
):
    rows, depth = xv.shape
    half = rows // 2
    kq = depth // KQ
    n1 = wg_hbm.shape[1] // B1
    n2 = wd_hbm.shape[1] // B2

    me = lax.axis_index("tp")
    core = lax.rem(me, 2)
    sibling = me + 1 - 2 * core
    across = lax.rem(me + 2, 4)
    mine = pl.multiple_of(core * half, half)
    theirs = pl.multiple_of((1 - core) * half, half)

    def x_copy(q):
        cols = pl.ds(q * kq, kq)
        return pltpu.make_async_copy(x_hbm.at[:, cols], xv.at[:, cols], x_sem.at[q])

    def up_copies(step, q):
        slot = lax.rem(step, RING)
        ks = pl.ds(q * kq, kq)
        cols = pl.ds(pl.multiple_of(step * B1, B1), B1)
        return (
            pltpu.make_async_copy(wg_hbm.at[ks, cols], wgv.at[slot, ks], g_sem.at[slot, q]),
            pltpu.make_async_copy(wu_hbm.at[ks, cols], wuv.at[slot, ks], u_sem.at[slot, q]),
        )

    def down_copy(j):
        cols = pl.ds(pl.multiple_of(j * B2, B2), B2)
        return pltpu.make_async_copy(wd_hbm.at[:, cols], wdv.at[j], d_sem.at[j])

    def pair_copy(j):
        return pltpu.make_async_remote_copy(
            src_ref=pair_out.at[j], dst_ref=pair_in.at[j],
            send_sem=ps_sem.at[j], recv_sem=pr_sem.at[j],
            device_id={"tp": sibling}, device_id_type=MESH,
        )

    def chip_copy(j):
        return pltpu.make_async_remote_copy(
            src_ref=chip_out.at[j], dst_ref=chip_in.at[j],
            send_sem=cs_sem.at[j], recv_sem=cr_sem.at[j],
            device_id={"tp": across}, device_id_type=MESH,
        )

    def y_copy(j):
        part = y_ref.at[pl.ds(mine, half), pl.ds(pl.multiple_of(j * B2, B2), B2)]
        return pltpu.make_async_remote_copy(
            src_ref=part, dst_ref=part,
            send_sem=ys_sem.at[j], recv_sem=yr_sem.at[j],
            device_id={"tp": sibling}, device_id_type=MESH,
        )

    for q in range(KQ):
        x_copy(q).start()
        for c in up_copies(0, q):
            c.start()
    for s in range(1, RING):
        for q in range(KQ):
            for c in up_copies(s, q):
                c.start()

    barrier = pltpu.get_barrier_semaphore()
    for peer in (sibling, across):
        pl.semaphore_signal(barrier, inc=1, device_id={"tp": peer}, device_id_type=MESH)

    def up_step(step, _):
        slot = lax.rem(step, RING)
        gate = up = None
        for q in range(KQ):
            @pl.when(step == 0)
            def _():
                x_copy(q).wait()

            for c in up_copies(step, q):
                c.wait()
            ks = pl.ds(q * kq, kq)
            g = jnp.dot(xv[:, ks], wgv[slot, ks], preferred_element_type=F32)
            u = jnp.dot(xv[:, ks], wuv[slot, ks], preferred_element_type=F32)
            gate = g if gate is None else gate + g
            up = u if up is None else up + u

        @pl.when(step + RING < n1)
        def _():
            for q in range(KQ):
                for c in up_copies(step + RING, q):
                    c.start()

        @pl.when(step + RING >= n1)
        def _():
            for i in range(n2 // RING):
                down_copy((step + RING - n1) * (n2 // RING) + i).start()

        cols = pl.ds(pl.multiple_of(step * B1, B1), B1)
        hid[:, cols] = (jax.nn.gelu(gate) * up).astype(BF16)
        return 0

    lax.fori_loop(0, n1, up_step, 0)
    pl.semaphore_wait(barrier, 2)

    def add_pair(j):
        pair_copy(j).wait_recv()
        total = term[j, pl.ds(mine, half), :] + pair_in[j].astype(F32)
        chip_out[j] = total.astype(BF16)
        chip_copy(j).start()

    def down_step(j, _):
        down_copy(j).wait()
        term[j] = jnp.dot(hid[...], wdv[j], preferred_element_type=F32)
        pair_out[j] = term[j, pl.ds(theirs, half), :].astype(BF16)
        pair_copy(j).start()

        @pl.when(j >= LAG)
        def _():
            add_pair(j - LAG)

        return 0

    lax.fori_loop(0, n2, down_step, 0)

    def rest_step(j, _):
        add_pair(j)
        return 0

    lax.fori_loop(n2 - LAG, n2, rest_step, 0)

    def y_step(j, _):
        chip_copy(j).wait_recv()
        total = chip_out[j].astype(F32) + chip_in[j].astype(F32)
        cols = pl.ds(pl.multiple_of(j * B2, B2), B2)
        y_ref[pl.ds(mine, half), cols] = total.astype(BF16)
        y_copy(j).start()
        return 0

    lax.fori_loop(0, n2, y_step, 0)

    def end_step(j, _):
        pair_copy(j).wait_send()
        chip_copy(j).wait_send()
        y_copy(j).wait()
        return 0

    lax.fori_loop(0, n2, end_step, 0)


def solution(mesh):
    def step(x, w_gate, w_up, w_down):
        rows, depth = x.shape
        ff = w_gate.shape[1]
        n2 = depth // B2
        dma = pltpu.SemaphoreType.DMA
        hbm = pl.BlockSpec(memory_space=pltpu.HBM)
        return pl.pallas_call(
            kernel,
            name="mlp",
            out_shape=jax.ShapeDtypeStruct((rows, depth), BF16),
            in_specs=[hbm] * 4,
            out_specs=pl.BlockSpec(memory_space=pltpu.VMEM),
            scratch_shapes=[
                pltpu.VMEM((rows, depth), BF16),
                pltpu.VMEM((RING, depth, B1), BF16),
                pltpu.VMEM((RING, depth, B1), BF16),
                pltpu.VMEM((n2, ff, B2), BF16),
                pltpu.VMEM((rows, ff), BF16),
                pltpu.VMEM((n2, rows, B2), F32),
                pltpu.VMEM((n2, rows // 2, B2), BF16),
                pltpu.VMEM((n2, rows // 2, B2), BF16),
                pltpu.VMEM((n2, rows // 2, B2), BF16),
                pltpu.VMEM((n2, rows // 2, B2), BF16),
                dma((KQ,)), dma((RING, KQ)), dma((RING, KQ)), dma((n2,)),
                dma((n2,)), dma((n2,)), dma((n2,)), dma((n2,)), dma((n2,)), dma((n2,)),
            ],
            compiler_params=pltpu.CompilerParams(
                collective_id=0, has_side_effects=True, vmem_limit_bytes=60 * 1024 * 1024
            ),
            cost_estimate=pl.CostEstimate(
                flops=6 * rows * depth * ff, bytes_accessed=6 * depth * ff, transcendentals=rows * ff
            ),
        )(x, w_gate, w_up, w_down)

    return jax.shard_map(
        step,
        mesh=mesh,
        in_specs=(P("dp", None), P(None, "tp"), P(None, "tp"), P("tp", None)),
        out_specs=P("dp", None),
        check_vma=False,
    )
```

```python
import jax
import jax.numpy as jnp
from jax import lax
from jax.experimental import pallas as pl
from jax.experimental.pallas import tpu as pltpu
from jax.sharding import PartitionSpec as P

MESH = pl.DeviceIdType.MESH
BF16 = jnp.bfloat16
F32 = jnp.float32

B1 = 256
RING = 4
LAST = 4
B2 = 256
WINDOW = 4
LAG = 2
PAIRS = 8


def kernel(
    x_hbm, wg_hbm, wu_hbm, wd_hbm, y_ref,
    xv, wgv, wuv, wdv, hid, term, pair_out, pair_in, chip_out, chip_in,
    x_sem, g_sem, u_sem, gl_sem, ul_sem, d_sem, pr_sem, cr_sem, yr_sem, send_sem,
):
    rows, depth = xv.shape
    half = rows // 2
    piece = depth // LAST
    n1 = wg_hbm.shape[1] // B1
    n2 = wd_hbm.shape[1] // B2

    me = lax.axis_index("tp")
    core = lax.rem(me, 2)
    sibling = me + 1 - 2 * core
    across = lax.rem(me + 2, 4)
    mine = pl.multiple_of(core * half, half)
    theirs = pl.multiple_of((1 - core) * half, half)

    x_copy = pltpu.make_async_copy(x_hbm, xv, x_sem)

    def up_copies(step):
        slot = lax.rem(step, RING)
        cols = pl.ds(pl.multiple_of(step * B1, B1), B1)
        return (
            pltpu.make_async_copy(wg_hbm.at[:, cols], wgv.at[slot], g_sem.at[slot]),
            pltpu.make_async_copy(wu_hbm.at[:, cols], wuv.at[slot], u_sem.at[slot]),
        )

    def last_copies(q):
        slot = (n1 - 1) % RING
        ks = pl.ds(q * piece, piece)
        cols = pl.ds((n1 - 1) * B1, B1)
        return (
            pltpu.make_async_copy(wg_hbm.at[ks, cols], wgv.at[slot, ks], gl_sem.at[q]),
            pltpu.make_async_copy(wu_hbm.at[ks, cols], wuv.at[slot, ks], ul_sem.at[q]),
        )

    def down_copy(j):
        cols = pl.ds(pl.multiple_of(j * B2, B2), B2)
        return pltpu.make_async_copy(wd_hbm.at[:, cols], wdv.at[j], d_sem.at[lax.rem(j, WINDOW)])

    def pair_copy(j):
        return pltpu.make_async_remote_copy(
            src_ref=pair_out.at[j], dst_ref=pair_in.at[j],
            send_sem=send_sem.at[0], recv_sem=pr_sem.at[lax.rem(j, PAIRS)],
            device_id={"tp": sibling}, device_id_type=MESH,
        )

    def chip_copy(j):
        return pltpu.make_async_remote_copy(
            src_ref=chip_out.at[j], dst_ref=chip_in.at[j],
            send_sem=send_sem.at[1], recv_sem=cr_sem.at[j],
            device_id={"tp": across}, device_id_type=MESH,
        )

    def y_copy(j):
        part = y_ref.at[pl.ds(mine, half), pl.ds(pl.multiple_of(j * B2, B2), B2)]
        return pltpu.make_async_remote_copy(
            src_ref=part, dst_ref=part,
            send_sem=send_sem.at[2], recv_sem=yr_sem,
            device_id={"tp": sibling}, device_id_type=MESH,
        )

    x_copy.start()
    for s in range(RING):
        for c in up_copies(s):
            c.start()

    barrier = pltpu.get_barrier_semaphore()
    for peer in (sibling, across):
        pl.semaphore_signal(barrier, inc=1, device_id={"tp": peer}, device_id_type=MESH)

    x_copy.wait()

    def up_step(step, _):
        slot = lax.rem(step, RING)
        for c in up_copies(step):
            c.wait()
        gate = jnp.dot(xv[...], wgv[slot], preferred_element_type=F32)
        up = jnp.dot(xv[...], wuv[slot], preferred_element_type=F32)

        @pl.when(step + RING < n1 - 1)
        def _():
            for c in up_copies(step + RING):
                c.start()

        @pl.when(step + RING == n1 - 1)
        def _():
            for q in range(LAST):
                for c in last_copies(q):
                    c.start()
            for j in range(WINDOW):
                down_copy(j).start(priority=1)

        cols = pl.ds(pl.multiple_of(step * B1, B1), B1)
        hid[:, cols] = (jax.nn.gelu(gate) * up).astype(BF16)
        return 0

    lax.fori_loop(0, n1 - 1, up_step, 0)

    slot = (n1 - 1) % RING
    gate = up = None
    for q in range(LAST):
        for c in last_copies(q):
            c.wait()
        ks = pl.ds(q * piece, piece)
        g = jnp.dot(xv[:, ks], wgv[slot, ks], preferred_element_type=F32)
        u = jnp.dot(xv[:, ks], wuv[slot, ks], preferred_element_type=F32)
        gate = g if gate is None else gate + g
        up = u if up is None else up + u
    hid[:, pl.ds((n1 - 1) * B1, B1)] = (jax.nn.gelu(gate) * up).astype(BF16)

    pl.semaphore_wait(barrier, 2)

    def add_pair(j):
        pair_copy(j).wait_recv()
        total = term[j, pl.ds(mine, half), :] + pair_in[j].astype(F32)
        chip_out[j] = total.astype(BF16)
        chip_copy(j).start()

    def down_step(j, _):
        down_copy(j).wait()

        @pl.when(j + WINDOW < n2)
        def _():
            down_copy(j + WINDOW).start(priority=1)

        term[j] = jnp.dot(hid[...], wdv[j], preferred_element_type=F32)
        pair_out[j] = term[j, pl.ds(theirs, half), :].astype(BF16)
        pair_copy(j).start()

        @pl.when(j >= LAG)
        def _():
            add_pair(j - LAG)

        return 0

    lax.fori_loop(0, n2, down_step, 0)

    def rest_step(j, _):
        add_pair(j)
        return 0

    lax.fori_loop(n2 - LAG, n2, rest_step, 0)

    def y_step(j, _):
        chip_copy(j).wait_recv()
        total = chip_out[j].astype(F32) + chip_in[j].astype(F32)
        cols = pl.ds(pl.multiple_of(j * B2, B2), B2)
        y_ref[pl.ds(mine, half), cols] = total.astype(BF16)
        y_copy(j).start()
        return 0

    lax.fori_loop(0, n2, y_step, 0)

    pltpu.make_async_copy(pair_out, pair_out, send_sem.at[0]).wait()
    pltpu.make_async_copy(chip_out, chip_out, send_sem.at[1]).wait()
    own = y_ref.at[pl.ds(mine, half)]
    pltpu.make_async_copy(own, own, send_sem.at[2]).wait()
    other = y_ref.at[pl.ds(theirs, half)]
    pltpu.make_async_copy(other, other, yr_sem).wait()


def solution(mesh):
    def step(x, w_gate, w_up, w_down):
        rows, depth = x.shape
        ff = w_gate.shape[1]
        n2 = depth // B2
        dma = pltpu.SemaphoreType.DMA
        hbm = pl.BlockSpec(memory_space=pltpu.HBM)
        return pl.pallas_call(
            kernel,
            name="mlp",
            out_shape=pltpu.VMEM((rows, depth), BF16),
            in_specs=[hbm] * 4,
            out_specs=pl.BlockSpec(memory_space=pltpu.VMEM),
            scratch_shapes=[
                pltpu.VMEM((rows, depth), BF16),
                pltpu.VMEM((RING, depth, B1), BF16),
                pltpu.VMEM((RING, depth, B1), BF16),
                pltpu.VMEM((n2, ff, B2), BF16),
                pltpu.VMEM((rows, ff), BF16),
                pltpu.VMEM((n2, rows, B2), F32),
                pltpu.VMEM((n2, rows // 2, B2), BF16),
                pltpu.VMEM((n2, rows // 2, B2), BF16),
                pltpu.VMEM((n2, rows // 2, B2), BF16),
                pltpu.VMEM((n2, rows // 2, B2), BF16),
                dma, dma((RING,)), dma((RING,)), dma((LAST,)), dma((LAST,)), dma((WINDOW,)),
                dma((PAIRS,)), dma((n2,)), dma, dma((3,)),
            ],
            compiler_params=pltpu.CompilerParams(
                collective_id=0, has_side_effects=True, vmem_limit_bytes=60 * 1024 * 1024
            ),
            cost_estimate=pl.CostEstimate(
                flops=6 * rows * depth * ff, bytes_accessed=6 * depth * ff, transcendentals=rows * ff
            ),
        )(x, w_gate, w_up, w_down)

    return jax.shard_map(
        step,
        mesh=mesh,
        in_specs=(P("dp", None), P(None, "tp"), P(None, "tp"), P("tp", None)),
        out_specs=P("dp", None),
        check_vma=False,
    )
```
